256 devices in a mesh: mp: 32 (over x, z), dp: 8 (over y, core).
Axes of the slice: x: 4, y: 4, z: 8, core: 2. Of those that a mesh axis runs over, the one named last changes fastest.
Arguments:
- tables: bfloat16 [20, 65536, 128], P(None, 'mp'), may hold values from -3 to 3
- block_rows: int32 [16384, 128], P(('mp', 'dp')), may hold values from 0 to 2047
- block_slots: int32 [16384, 128], P(('mp', 'dp')), may hold values from 0 to 127
- block_table: int32 [16384], P(('mp', 'dp')), may hold values from 0 to 19
- block_peer: int32 [16384, 1], P(('mp', 'dp')), may hold values from 0 to 31; in each aligned block of 64 rows (0 to 63, 64 to 127, ...) at most 4 rows name the same one
- block_len: int32 [16384], P(('mp', 'dp')), may hold values from 1 to 128
- block_count: int32 [256], P(('mp', 'dp')), may hold values from 1 to 64, as said below
- cross_in: bfloat16 [4, 2560, 256], P(None, 'dp'), may hold values from -0.23632812 to 0.23632812
- cross_mix: bfloat16 [4, 256, 256], replicated, may hold values from -0.5625 to 0.5625
- cross_out: bfloat16 [4, 256, 2560], P(None, None, 'dp'), may hold values from -0.375 to 0.375
- cross_bias: float32 [4, 2560], replicated, may hold values from -3 to 3
- gate_weight: bfloat16 [4, 2560], replicated, may hold values from -0.47265625 to 0.47265625
Outputs:
- crossed: bfloat16 [32768, 2560], P(('mp', 'dp'))
The draws below stay inside these ranges and needn't reach their ends.
Inputs may be any that keep to these rules, and one draw needn't show every extreme that they name: `block_peer`: in the 64 blocks of one device no destination is named by more than 4 blocks, a bound that the blocks of some device reach. The live blocks of a device are its first block_count blocks; some device has exactly 64. Entries of a block at positions below its block_len are live. `block_rows`: A row index within the device's own shard of the table. `block_slots`: A sample of the destination device.
All inputs are finite; a program needn't handle non-finite values.
Results may differ from the reference program's by a relative error of at most 0.0059.
Values may be sent and summed in bfloat16 or wider, within the bound.
A program may use at most 128 MiB of HBM per device.

```python
import math
import jax
import jax.numpy as jnp
import numpy as np
from jax import lax

WIDTH = 128
TABLES = 20
ROWS_DEV = 2048
BLOCK = 128
NBLK = 64
B_DEV = 128
RANK = 256
EXPERTS = 4
D = 2560
CAP = 4
N_MP = 32
N_DP = 8


def draw_block_count(key, part):
    devices = N_MP * N_DP
    heavy = jax.random.randint(jax.random.fold_in(key, 11), (devices,), 0, 8) == 0
    high = jax.random.randint(jax.random.fold_in(key, 12), (devices,), NBLK // 2, NBLK + 1)
    low = jax.random.randint(jax.random.fold_in(key, 13), (devices,), max(1, NBLK // 8), NBLK // 2 + 1)
    counts = jnp.where(heavy, high, low)
    chosen = jax.random.randint(jax.random.fold_in(key, 14), (), 0, devices)
    return counts.at[chosen].set(NBLK).astype(jnp.int32)


def touch_ends(values, own_key, least, largest):
    extent = values.shape
    place = [jax.random.randint(jax.random.fold_in(own_key, axis), (), 0, extent[axis]) for axis in range(len(extent))]
    values = values.at[tuple(place)].set(least)
    longest = extent.index(max(extent))
    place[longest] = (place[longest] + 1) % extent[longest]
    return values.at[tuple(place)].set(largest)


def block_levels(key, extent, cuts, smallest, top_value):
    loudness = 1.0
    for dim, blocks in cuts:
        draws = jax.random.uniform(jax.random.fold_in(jax.random.fold_in(key, 6), dim), (blocks,), jnp.float32, smallest / len(cuts), top_value / len(cuts))
        loudness = loudness * jnp.repeat(jnp.exp(draws), extent[dim] // blocks).reshape((-1,) + (1,) * (len(extent) - 1 - dim))
    return loudness


def routed_block(key, own, number, rows, amount, top, bound, slope):
    order = jax.random.permutation(key, amount)
    packed, common = load_shares(amount, rows * top, bound, slope, True), load_shares(amount, rows * top, bound, slope, False)
    places = jnp.arange(amount)

    def named(tallies, rotation):
        used = int((tallies > 0).sum())
        fixed = max(1, used // 4)
        passed = fixed + (places - fixed + rotation * (used - fixed)) % max(1, amount - fixed)
        return jnp.zeros((amount,), jnp.int32).at[order[jnp.where(places < fixed, places, passed)]].set(jnp.asarray(tallies, jnp.int32))

    tallies = jnp.where(number % 4 == 0, named(packed, number // 4), named(common, number - number // 4 - 1))
    mixed = jax.random.permutation(jax.random.fold_in(own, 3), amount)
    donor, receiver = mixed[0:amount // 2 * 2:2], mixed[1:amount // 2 * 2:2]
    margin = jnp.minimum(tallies[donor] - 1, bound - tallies[receiver]) // 2
    margin = jnp.where((donor == order[0]) | (receiver == order[0]) | (tallies[receiver] == 0), 0, jnp.maximum(margin, 0))
    passed = jax.random.randint(jax.random.fold_in(own, 4), (amount // 2,), 0, 1 << 20) % (margin + 1)
    tallies = tallies.at[donor].add(-passed).at[receiver].add(passed)
    labels = jnp.searchsorted(jnp.cumsum(tallies), jnp.arange(rows * top), side="right").astype(jnp.int32)
    grid = labels.reshape(top, rows).T
    grid = grid[jax.random.permutation(jax.random.fold_in(own, 1), rows)]
    rotation = jax.random.randint(jax.random.fold_in(own, 2), (rows, 1), 0, top)
    return jnp.take_along_axis(grid, (jnp.arange(top)[None, :] + rotation) % top, axis=1)


def load_shares(count, total, reach, skew, full):
    weights = [(1 << 20) // math.isqrt(standing ** skew) + 1 for standing in range(1, count + 1)]
    largest = reach if full else min(reach, max(-(-total // count), total * weights[0] // sum(weights)))
    least = 1 if total - largest >= count - 1 else 0
    given, surplus = [largest] + [least] * (count - 1), total - largest - least * (count - 1)
    while surplus > 0:
        free = [i for i in range(1, count) if given[i] < largest] or [i for i in range(1, count) if given[i] < reach]
        whole, budget = sum([weights[i] for i in free]), surplus
        for i in free:
            extra = min(reach - given[i], max(1, budget * weights[i] // whole), surplus)
            given[i] = given[i] + extra
            surplus = surplus - extra
    return np.array(given)


def normal_values(stream_key, dims, deviation, limit, shards=(), kind=jnp.bfloat16):
    level = block_levels(stream_key, dims, shards, -0.22, 0.18) if shards else 1.0
    values = jax.random.normal(stream_key, dims, jnp.float32) * deviation * level
    return jnp.minimum(jnp.maximum(values, -limit), limit).astype(kind)


def setup_inputs(seed: int = 0) -> dict:
    key_list = jax.random.split(jax.random.key(seed), 13)
    tables = normal_values(key_list[0], (TABLES, ROWS_DEV * N_MP, WIDTH), 0.5, 3.0, ((1, 32),))
    block_rows = touch_ends(jax.random.randint(key_list[1], (N_MP * N_DP * NBLK, BLOCK), 0, ROWS_DEV), jax.random.fold_in(key_list[1], 1), 0, ROWS_DEV - 1).astype(jnp.int32)
    block_slots = touch_ends(jax.random.randint(key_list[2], (N_MP * N_DP * NBLK, BLOCK), 0, B_DEV), jax.random.fold_in(key_list[2], 1), 0, B_DEV - 1).astype(jnp.int32)
    block_table = touch_ends(jax.random.randint(key_list[3], (N_MP * N_DP * NBLK,), 0, TABLES), jax.random.fold_in(key_list[3], 1), 0, TABLES - 1).astype(jnp.int32)
    block_peer_keys = jax.random.split(jax.random.fold_in(key_list[4], 1), (N_MP * N_DP * NBLK) // NBLK)
    block_peer_turns = jax.random.permutation(jax.random.fold_in(key_list[4], 3), (N_MP * N_DP * NBLK) // NBLK)
    block_peer = jax.vmap(lambda own, number: routed_block(jax.random.fold_in(key_list[4], 2), own, number, NBLK, N_MP, 1, CAP, 2))(block_peer_keys, block_peer_turns).reshape((N_MP * N_DP * NBLK, 1))
    block_len = touch_ends(jax.random.randint(key_list[5], (N_MP * N_DP * NBLK,), 1, BLOCK + 1), jax.random.fold_in(key_list[5], 1), 1, BLOCK).astype(jnp.int32)
    block_count = draw_block_count(jax.random.fold_in(key_list[12], 71), 0)
    cross_in = normal_values(key_list[7], (EXPERTS, D, RANK), (2.0 / D ** 0.5), 0.23632812, ((1, 8),))
    cross_mix = normal_values(key_list[8], (EXPERTS, RANK, RANK), (1.5 / RANK ** 0.5), 0.5625)
    cross_out = normal_values(key_list[9], (EXPERTS, RANK, D), RANK ** -0.5, 0.375, ((2, 8),))
    cross_bias = normal_values(key_list[10], (EXPERTS, D), 0.5, 3.0, (), jnp.float32)
    gate_weight = normal_values(key_list[11], (EXPERTS, D), (4.0 / D ** 0.5), 0.47265625)
    return {"tables": tables, "block_rows": block_rows, "block_slots": block_slots, "block_table": block_table, "block_peer": block_peer, "block_len": block_len, "block_count": block_count, "cross_in": cross_in, "cross_mix": cross_mix, "cross_out": cross_out, "cross_bias": cross_bias, "gate_weight": gate_weight}


def reference(tables, block_rows, block_slots, block_table, block_peer, block_len, block_count, cross_in, cross_mix, cross_out, cross_bias, gate_weight):
    devices = N_MP * N_DP
    rows_all = block_rows.reshape(devices, NBLK, BLOCK)
    slots_all = block_slots.reshape(devices, NBLK, BLOCK)
    table_all = block_table.reshape(devices, NBLK)
    peer_all = block_peer.reshape(devices, NBLK)
    length_all = block_len.reshape(devices, NBLK)
    entries = jnp.arange(BLOCK, dtype=jnp.int32)
    blocks = jnp.arange(NBLK, dtype=jnp.int32)

    def one_device(index, total):
        shard = index // N_DP
        group = index % N_DP
        live = (blocks[:, None] < block_count[index]) & (entries[None, :] < length_all[index][:, None])
        table_ids = jnp.broadcast_to(table_all[index][:, None], (NBLK, BLOCK)).astype(jnp.int32)
        peer_ids = jnp.broadcast_to(peer_all[index][:, None], (NBLK, BLOCK)).astype(jnp.int32)
        row_ids = (rows_all[index] + shard * ROWS_DEV).astype(jnp.int32)
        values = tables[table_ids, row_ids].astype(jnp.float32) * live[:, :, None].astype(jnp.float32)
        partial_value = jnp.zeros((N_MP, TABLES, B_DEV, WIDTH), jnp.float32)
        partial_value = partial_value.at[peer_ids, table_ids, slots_all[index]].add(values)
        rounded = lax.optimization_barrier(partial_value.astype(jnp.bfloat16)).astype(jnp.float32)
        return total.at[:, group].add(rounded)

    total = lax.fori_loop(0, devices, one_device, jnp.zeros((N_MP, N_DP, TABLES, B_DEV, WIDTH), jnp.float32))
    embedded = total.transpose(0, 1, 3, 2, 4).reshape(devices * B_DEV, TABLES * WIDTH).astype(jnp.bfloat16)
    gate = jax.nn.sigmoid(jnp.dot(embedded, gate_weight.T, preferred_element_type=jnp.float32))
    weighted = jnp.zeros(embedded.shape, jnp.float32)
    for expert in range(EXPERTS):
        hidden = jnp.tanh(jnp.dot(embedded, cross_in[expert], preferred_element_type=jnp.float32)).astype(jnp.bfloat16)
        mixed = jnp.tanh(jnp.dot(hidden, cross_mix[expert], preferred_element_type=jnp.float32)).astype(jnp.bfloat16)
        expand = jnp.dot(mixed, cross_out[expert], preferred_element_type=jnp.float32) + cross_bias[expert][None, :]
        weighted = weighted + gate[:, expert][:, None] * expand
    base = embedded.astype(jnp.float32)
    return (base + base * weighted).astype(jnp.bfloat16)
```

```python
import functools

import jax
import jax.numpy as jnp
from jax import lax
from jax.experimental import pallas as pl
from jax.experimental.pallas import tpu as pltpu
from jax.sharding import PartitionSpec as P

MESH = pl.DeviceIdType.MESH
CAP = 4
META = 16
RCHUNK = 512


def exchange_kernel(
    peers,
    tab_ref,
    tables_hbm,
    rows_ref,
    slots_ref,
    meta_ref,
    win_hbm,
    wout_hbm,
    recv_hbm,
    win_all,
    wout_all,
    tables_v,
    sbuf,
    table_sem,
    send_sem,
    recv_sem,
    own_sem,
    wsend,
    wrecv,
    wown,
):
    m = lax.axis_index("mp")
    d = lax.axis_index("dp")
    table_count, rows_dev, width = tables_v.shape
    entries = rows_ref.shape[0]
    samples = entries
    y, c = lax.div(d, 2), lax.rem(d, 2)
    up = lax.rem(y + 1, 4) * 2 + c
    dn = lax.rem(y + 3, 4) * 2 + c
    opp = lax.rem(y + 2, 4) * 2 + c
    mate = y * 2 + 1 - c

    table_copy = pltpu.make_async_copy(tables_hbm, tables_v, table_sem)
    table_copy.start()

    def wcopy(src, dst, sem, target):
        return pltpu.make_async_remote_copy(
            src_ref=src,
            dst_ref=dst,
            send_sem=wsend.at[sem],
            recv_sem=wrecv.at[sem],
            device_id={"mp": m, "dp": target},
            device_id_type=MESH,
        )

    pairs = ((win_hbm, win_all), (wout_hbm, wout_all))
    half = win_hbm.shape[0] // 2
    first = []
    for a, (src, dst) in enumerate(pairs):
        for s, target in enumerate((up, dn, mate)):
            first.append(wcopy(src, dst.at[d], a * 8 + s, target))
    for copy in first:
        copy.start()
    own_w = [pltpu.make_async_copy(src, dst.at[d], wown.at[a]) for a, (src, dst) in enumerate(pairs)]
    for copy in own_w:
        copy.start()
    table_copy.wait()

    lane = lax.broadcasted_iota(jnp.int32, (entries, entries), 1).astype(jnp.float32)
    sub = lax.broadcasted_iota(jnp.int32, (samples, entries), 0).astype(jnp.float32)
    wide = lax.broadcasted_iota(jnp.int32, (entries, RCHUNK), 1).astype(jnp.float32)

    def send(step):
        p = lax.rem(m + step, peers)
        return pltpu.make_async_remote_copy(
            src_ref=sbuf.at[p],
            dst_ref=recv_hbm.at[m],
            send_sem=send_sem.at[step],
            recv_sem=recv_sem.at[step],
            device_id={"mp": p, "dp": d},
            device_id_type=MESH,
        )

    def fill(step):
        p = lax.rem(m + step, peers)
        for j in range(CAP):
            slot = p * CAP + j
            column = jnp.sum(
                jnp.where(lane == slot.astype(jnp.float32), rows_ref[...], 0.0), axis=1, keepdims=True
            )
            table = tab_ref[slot]
            picked = jnp.zeros((entries, width), jnp.float32)
            for part in range(rows_dev // RCHUNK):
                hot = jnp.where(column - float(part * RCHUNK) == wide, 1.0, 0.0).astype(jnp.bfloat16)
                picked += jnp.dot(
                    hot,
                    tables_v[table, part * RCHUNK : (part + 1) * RCHUNK, :],
                    preferred_element_type=jnp.float32,
                )
            pool = jnp.where(slots_ref[pl.ds(slot, 1), :] == sub, 1.0, 0.0).astype(jnp.bfloat16)
            pooled = jnp.dot(pool, picked.astype(jnp.bfloat16), preferred_element_type=jnp.float32)
            sbuf[p, j * samples : (j + 1) * samples, :] = pooled.astype(jnp.bfloat16)
        sbuf[p, CAP * samples :, :] = meta_ref[p]

    def body(step, carry):
        fill(step)

        @pl.when(step >= 2)
        def _():
            send(step - 1).start()

        return carry

    lax.fori_loop(1, peers, body, 0)
    fill(jnp.int32(0))
    send(peers - 1).start()
    own = pltpu.make_async_copy(sbuf.at[m], recv_hbm.at[m], own_sem)
    own.start()

    second = []
    for a, (src, dst) in enumerate(pairs):
        wcopy(src, dst.at[dn], a * 8 + 0, up).wait_recv()
        wcopy(src, dst.at[up], a * 8 + 1, dn).wait_recv()
        second.append(wcopy(dst.at[dn, :half], dst.at[dn, :half], a * 8 + 3, up))
        second.append(wcopy(dst.at[up, half:], dst.at[up, half:], a * 8 + 4, dn))
        second.append(wcopy(dst.at[dn], dst.at[dn], a * 8 + 5, mate))
        second.append(wcopy(dst.at[up], dst.at[up], a * 8 + 6, mate))
    for copy in second:
        copy.start()
    third = []
    for a, (src, dst) in enumerate(pairs):
        wcopy(dst.at[opp, :half], dst.at[opp, :half], a * 8 + 3, up).wait_recv()
        wcopy(dst.at[opp, half:], dst.at[opp, half:], a * 8 + 4, dn).wait_recv()
        third.append(wcopy(dst.at[opp], dst.at[opp], a * 8 + 7, mate))
    for copy in third:
        copy.start()
    for a, (src, dst) in enumerate(pairs):
        for s in (2, 5, 6, 7):
            wcopy(src, dst.at[mate], a * 8 + s, mate).wait_recv()
    for copy in first + second + third:
        copy.wait_send()
    for copy in own_w:
        copy.wait()

    def finish(step, carry):
        copy = send(step)
        copy.wait_send()
        q = lax.rem(m + peers - step, peers)
        pltpu.make_async_remote_copy(
            src_ref=sbuf.at[m],
            dst_ref=recv_hbm.at[q],
            send_sem=send_sem.at[step],
            recv_sem=recv_sem.at[step],
            device_id={"mp": q, "dp": d},
            device_id_type=MESH,
        ).wait_recv()
        return carry

    lax.fori_loop(1, peers, finish, 0)
    own.wait()


def exchange(tables, tab_slot, rows_t, slot_code, meta, cross_in, cross_out, peers):
    table_count, rows_dev, width = tables.shape
    entries = rows_t.shape[0]
    dp = lax.axis_size("dp")
    packed = CAP * entries + META
    hbm = pl.BlockSpec(memory_space=pl.ANY)
    vmem = pl.BlockSpec(memory_space=pltpu.VMEM)
    return pl.pallas_call(
        functools.partial(exchange_kernel, peers),
        out_shape=(
            jax.ShapeDtypeStruct((peers, packed, width), jnp.bfloat16),
            jax.ShapeDtypeStruct((dp,) + cross_in.shape, jnp.bfloat16),
            jax.ShapeDtypeStruct((dp,) + cross_out.shape, jnp.bfloat16),
        ),
        in_specs=[pl.BlockSpec(memory_space=pltpu.SMEM), hbm, vmem, vmem, vmem, hbm, hbm],
        out_specs=(hbm, hbm, hbm),
        scratch_shapes=[
            pltpu.VMEM((table_count, rows_dev, width), jnp.bfloat16),
            pltpu.VMEM((peers, packed, width), jnp.bfloat16),
            pltpu.SemaphoreType.DMA,
            pltpu.SemaphoreType.DMA((peers,)),
            pltpu.SemaphoreType.DMA((peers,)),
            pltpu.SemaphoreType.DMA,
            pltpu.SemaphoreType.DMA((16,)),
            pltpu.SemaphoreType.DMA((16,)),
            pltpu.SemaphoreType.DMA((2,)),
        ],
        compiler_params=pltpu.CompilerParams(has_side_effects=True, vmem_limit_bytes=60 * 1024 * 1024),
        name="exchange",
    )(tab_slot, tables, rows_t, slot_code, meta, cross_in, cross_out)


def cross_kernel(
    tab_ref,
    recv_ref,
    mix_ref,
    bias_ref,
    gate_ref,
    win_hbm,
    wout_hbm,
    out_ref,
    acc,
    win_v,
    wout_v,
    sems,
):
    peers = recv_ref.shape[0]
    samples, wide = acc.shape
    width = recv_ref.shape[2]
    dp, experts, cols, rank = win_v.shape
    in_copy = pltpu.make_async_copy(win_hbm, win_v, sems.at[0])
    out_copy = pltpu.make_async_copy(wout_hbm, wout_v, sems.at[1])
    in_copy.start()
    out_copy.start()
    acc[...] = jnp.zeros_like(acc)

    def add(q, carry):
        for j in range(CAP):
            table = tab_ref[q, j] - 1

            @pl.when(table >= 0)
            def _():
                col = pl.ds(pl.multiple_of(table * width, width), width)
                acc[:, col] += recv_ref[q, j * samples : (j + 1) * samples, :].astype(jnp.float32)

        return carry

    lax.fori_loop(0, peers, add, 0)
    embedded = acc[...].astype(jnp.bfloat16)
    gate = jax.nn.sigmoid(
        lax.dot_general(embedded, gate_ref[...], (((1,), (1,)), ((), ())), preferred_element_type=jnp.float32)
    )
    in_copy.wait()
    mixed = []
    for e in range(experts):
        projected = jnp.zeros((samples, rank), jnp.float32)
        for k in range(dp):
            projected += jnp.dot(
                embedded[:, k * cols : (k + 1) * cols], win_v[k, e], preferred_element_type=jnp.float32
            )
        hidden = jnp.tanh(projected).astype(jnp.bfloat16)
        mixed.append(
            jnp.tanh(jnp.dot(hidden, mix_ref[e], preferred_element_type=jnp.float32)).astype(jnp.bfloat16)
        )
    out_copy.wait()
    for k in range(dp):
        span = slice(k * cols, (k + 1) * cols)
        weighted = jnp.zeros((samples, cols), jnp.float32)
        for e in range(experts):
            grown = jnp.dot(mixed[e], wout_v[k, e], preferred_element_type=jnp.float32)
            weighted += gate[:, e : e + 1] * (grown + bias_ref[e : e + 1, span])
        base = embedded[:, span].astype(jnp.float32)
        out_ref[:, span] = (base + base * weighted).astype(jnp.bfloat16)


def cross(recv, tabs, win_all, wout_all, cross_mix, cross_bias, gate_weight):
    peers, packed, width = recv.shape
    samples = (packed - META) // CAP
    wide = cross_bias.shape[1]
    hbm = pl.BlockSpec(memory_space=pl.ANY)
    vmem = pl.BlockSpec(memory_space=pltpu.VMEM)
    return pl.pallas_call(
        cross_kernel,
        out_shape=jax.ShapeDtypeStruct((samples, wide), jnp.bfloat16),
        in_specs=[pl.BlockSpec(memory_space=pltpu.SMEM), vmem, vmem, vmem, vmem, hbm, hbm],
        out_specs=vmem,
        scratch_shapes=[
            pltpu.VMEM((samples, wide), jnp.float32),
            pltpu.VMEM(win_all.shape, jnp.bfloat16),
            pltpu.VMEM(wout_all.shape, jnp.bfloat16),
            pltpu.SemaphoreType.DMA((2,)),
        ],
        compiler_params=pltpu.CompilerParams(vmem_limit_bytes=60 * 1024 * 1024),
        name="cross",
    )(tabs, recv, cross_mix, cross_bias, gate_weight, win_all, wout_all)


def on_device(
    tables,
    block_rows,
    block_slots,
    block_table,
    block_peer,
    block_len,
    block_count,
    cross_in,
    cross_mix,
    cross_out,
    cross_bias,
    gate_weight,
):
    peers = lax.axis_size("mp")
    blocks, entries = block_rows.shape
    ids = jnp.arange(blocks, dtype=jnp.int32)
    live = ids < block_count[0]
    peer = block_peer[:, 0]
    earlier = (peer[:, None] == peer[None, :]) & (ids[None, :] < ids[:, None])
    position = jnp.sum(earlier.astype(jnp.int32), axis=1)
    target = jnp.where(live, peer * CAP + position, -1)
    pick = target[None, :] == jnp.arange(peers * CAP, dtype=jnp.int32)[:, None]
    tab_code = jnp.sum(jnp.where(pick, block_table[None, :] + 1, 0), axis=1)
    live_entry = jnp.arange(entries, dtype=jnp.int32)[None, :] < block_len[:, None]
    row_code = jnp.where(live_entry, block_rows + 1, 0)
    slot_code = jnp.where(live_entry, block_slots + 1, 0)
    rows_t = jnp.sum(jnp.where(pick.T[:, None, :], row_code[:, :, None], 0), axis=0) - 1
    slots_s = jnp.sum(jnp.where(pick[:, :, None], slot_code[None, :, :], 0), axis=1) - 1
    meta = jnp.pad(
        tab_code.reshape(peers, 1, CAP).astype(jnp.bfloat16), ((0, 0), (0, META - 1), (0, tables.shape[2] - CAP))
    )
    recv, win_all, wout_all = exchange(
        tables,
        jnp.maximum(tab_code - 1, 0),
        rows_t.astype(jnp.float32),
        slots_s.astype(jnp.float32),
        meta,
        cross_in,
        cross_out,
        peers,
    )
    tabs = recv[:, CAP * B_DEV, :CAP].astype(jnp.int32)
    return cross(recv, tabs, win_all, wout_all, cross_mix, cross_bias, gate_weight)


B_DEV = 128


def solution(mesh):
    in_specs = (
        P(None, "mp", None),
        P(("mp", "dp"), None),
        P(("mp", "dp"), None),
        P(("mp", "dp")),
        P(("mp", "dp"), None),
        P(("mp", "dp")),
        P(("mp", "dp")),
        P(None, "dp", None),
        P(),
        P(None, None, "dp"),
        P(),
        P(),
    )
    out_specs = P(("mp", "dp"), None)
    return jax.shard_map(
        on_device, mesh=mesh, in_specs=in_specs, out_specs=out_specs, check_vma=False
    )
```

```python
import functools

import jax
import jax.numpy as jnp
from jax import lax
from jax.experimental import pallas as pl
from jax.experimental.pallas import tpu as pltpu
from jax.sharding import PartitionSpec as P

MESH = pl.DeviceIdType.MESH
F32, BF16 = jnp.float32, jnp.bfloat16
CAP = 4
META = 8
TIGHT = 320
RCHUNK = 512
LIMIT = 60 * 1024 * 1024


def iota(shape, axis):
    return lax.broadcasted_iota(jnp.int32, shape, axis).astype(F32)


def dot(a, b):
    return jnp.dot(a, b, preferred_element_type=F32)


def dot_t(a, b):
    return lax.dot_general(a, b, (((1,), (1,)), ((), ())), preferred_element_type=F32)


def dot_l(a, b):
    return lax.dot_general(a, b, (((0,), (0,)), ((), ())), preferred_element_type=F32)


def hot(mask):
    return jnp.where(mask, 1.0, 0.0).astype(BF16)


def prep_kernel(
    tight, count_ref, rows_ref, slots_ref, table_ref, peer_ref, len_ref, tab_o, rows_o, slots_o, qh_o, ql_o, meta_o, need_o, used
):
    blocks, entries = rows_ref.shape
    slots_n = rows_o.shape[1]
    count = count_ref[0].astype(F32)
    k_sub, k_lane = iota((blocks, blocks), 0), iota((blocks, blocks), 1)
    eye = k_sub == k_lane

    def column(row):
        return jnp.sum(jnp.where(eye, row, 0.0), axis=1, keepdims=True)

    table_r, peer_r = table_ref[...].astype(F32), peer_ref[...].astype(F32)
    table_c, peer_c, len_c = column(table_r), column(peer_r), column(len_ref[...].astype(F32))
    live_r, live_c = k_lane[:1] < count, k_sub[:, :1] < count
    same = peer_c == peer_r
    before = same & (k_lane < k_sub)
    alike = same & (column(table_r) == table_r) & live_r & live_c
    follows_c = jnp.max(jnp.where(alike & (k_lane < k_sub), 1.0, 0.0), axis=1, keepdims=True)
    follows_r = jnp.max(jnp.where(alike & (k_sub < k_lane), 1.0, 0.0), axis=0, keepdims=True)
    leads_c = jnp.where(live_c, 1.0 - follows_c, 0.0)
    pos_c = jnp.sum(jnp.where(before, 1.0, 0.0), axis=1, keepdims=True)
    pos_r = jnp.sum(jnp.where(same & (k_sub < k_lane), 1.0, 0.0), axis=0, keepdims=True)
    target_r = jnp.where(live_r, peer_r * CAP + pos_r, -1.0)
    target_c = jnp.where(live_c, peer_c * CAP + pos_c, -1.0)
    place = hot(iota((slots_n, blocks), 0) == target_r)
    place_t = hot(target_c == iota((blocks, slots_n), 1))

    live_entry = (iota((blocks, entries), 1) < len_c) & live_c
    slot_code = jnp.where(live_entry, slots_ref[...].astype(F32) + 1.0, 0.0)
    slots_o[...] = dot(place, slot_code.astype(BF16)) - 1.0
    row_code = jnp.where(live_entry, rows_ref[...].astype(F32) + 1.0, 0.0)
    high = jnp.floor(row_code * (1.0 / 64.0))
    low = row_code - 64.0 * high
    rows_o[...] = 64.0 * dot_l(high.astype(BF16), place_t) + dot_l(low.astype(BF16), place_t) - 1.0
    tab_o[...] = dot(jnp.broadcast_to(table_r, (8, blocks)).astype(BF16), place_t).astype(jnp.int32)

    lanes = iota((entries, entries), 1)
    if tight:
        slot_t = slot_code.T - 1.0
        for k in range(blocks):
            touched = jnp.where(slot_t[:, k : k + 1] == lanes, 1.0, 0.0)
            used[k : k + 1, :] = jnp.minimum(jnp.sum(touched, axis=0, keepdims=True), 1.0)
        taken = leads_c * jnp.minimum(dot(hot(alike), used[...].astype(BF16)), 1.0)
    else:
        taken = leads_c + jnp.zeros((blocks, entries), F32)
    rank = dot(taken.astype(BF16), hot(iota((entries, entries), 0) < lanes))
    amount_c = jnp.sum(taken, axis=1, keepdims=True)
    amount_r = jnp.sum(jnp.where(eye, amount_c, 0.0), axis=0, keepdims=True)
    off_c = jnp.sum(jnp.where(before, amount_r, 0.0), axis=1, keepdims=True)
    need_o[...] = jnp.zeros_like(need_o) + jnp.max(jnp.where(live_c, off_c + amount_c, 0.0))

    spot = jnp.where(taken > 0.0, off_c + rank + 1.0, 0.0)
    spot_high = jnp.floor(spot * (1.0 / 64.0))
    spot_low = spot - 64.0 * spot_high
    led = hot(alike & (follows_r == 0.0))
    qh_o[...] = dot(place, dot(led, spot_high.astype(BF16)).astype(BF16))
    ql_o[...] = dot(place, dot(led, spot_low.astype(BF16)).astype(BF16))

    off_high = jnp.floor(off_c * (1.0 / 16.0))
    lane_e = iota((blocks, entries), 1)
    facts = jnp.where(lane_e == 0.0, table_c + 1.0, jnp.where(lane_e == 1.0, off_high, off_c - 16.0 * off_high))
    facts = jnp.where(lane_e < 3.0, leads_c * facts, 0.0)
    line = lax.broadcasted_iota(jnp.int32, (meta_o.shape[0], blocks), 0)
    pair, part = (line >> 3) * CAP, line & 7
    rank_line = hot(jnp.where(part < CAP, pair + part, -2).astype(F32) == target_r)
    fact_line = hot(jnp.where((part >= CAP) & (part < 2 * CAP), pair + part - CAP, -2).astype(F32) == target_r)
    meta = dot(rank_line, (taken * (rank + 1.0)).astype(BF16)) + dot(fact_line, facts.astype(BF16))
    meta_o[...] = meta.astype(BF16)


def prep(tight, peers, count, rows, slots, table, peer, length):
    blocks, entries = rows.shape
    slots_n = peers * CAP
    vmem = pl.BlockSpec(memory_space=pltpu.VMEM)
    return pl.pallas_call(
        functools.partial(prep_kernel, tight),
        out_shape=(
            jax.ShapeDtypeStruct((8, slots_n), jnp.int32),
            jax.ShapeDtypeStruct((entries, slots_n), F32),
            jax.ShapeDtypeStruct((slots_n, entries), F32),
            jax.ShapeDtypeStruct((slots_n, entries), F32),
            jax.ShapeDtypeStruct((slots_n, entries), F32),
            jax.ShapeDtypeStruct((peers * META, entries), BF16),
            jax.ShapeDtypeStruct((8, entries), F32),
        ),
        in_specs=[pl.BlockSpec(memory_space=pltpu.SMEM)] + [vmem] * 5,
        out_specs=(vmem,) * 7,
        scratch_shapes=[pltpu.VMEM((blocks, entries), F32)],
        name="prep_tight" if tight else "prep_full",
    )(count, rows, slots, table, peer, length)


def exchange_kernel(tight, peers, *refs):
    if tight:
        (tab_ref, tables_hbm, rows_ref, slots_ref, qh_ref, ql_ref, meta_ref, need_ref, win_hbm, wout_hbm) = refs[:10]
        (got_ref, facts_ref, flag_ref, win_all, wout_all) = refs[10:15]
        (tables_v, sbuf, rbuf, table_sem, send_sem, recv_sem) = refs[15:21]
        (mp_need, dp_need, mine, nsend, nrecv, dsend, drecv, wsend, wrecv, wown) = refs[21:]
    else:
        (tab_ref, tables_hbm, rows_ref, slots_ref, qh_ref, ql_ref, meta_ref) = refs[:7]
        (got_ref, facts_ref) = refs[7:9]
        (tables_v, sbuf, rbuf, table_sem, send_sem, recv_sem) = refs[9:]
    m = lax.axis_index("mp")
    d = lax.axis_index("dp")
    table_count, rows_dev, width = tables_v.shape
    entries = rows_ref.shape[0]
    samples = entries
    space = sbuf.shape[1] - META
    x, z = lax.div(m, 8), lax.rem(m, 8)
    self_step = 28

    def shift(step):
        turn = lax.div(step, 4)
        half = lax.div(turn, 2)
        dz = jnp.where(lax.rem(turn, 2) == 0, 4 + half, 3 - half)
        return lax.rem(step, 4), dz

    def ahead(step):
        dx, dz = shift(step)
        return lax.rem(x + dx, 4) * 8 + lax.rem(z + dz, 8)

    def behind(step):
        dx, dz = shift(step)
        return lax.rem(x + 4 - dx, 4) * 8 + lax.rem(z + 8 - dz, 8)

    table_copy = pltpu.make_async_copy(tables_hbm, tables_v, table_sem)
    table_copy.start()

    barrier = pltpu.get_barrier_semaphore()

    def greet(step, carry):
        pl.semaphore_signal(
            barrier, inc=1, device_id={"mp": lax.rem(m + step, peers), "dp": d}, device_id_type=MESH
        )
        return carry

    lax.fori_loop(1, peers, greet, 0)
    if tight:
        for step in range(1, 8):
            pl.semaphore_signal(
                barrier, inc=1, device_id={"mp": m, "dp": lax.rem(d + step, 8)}, device_id_type=MESH
            )
        pl.semaphore_wait(barrier, peers - 1 + 7)
    else:
        pl.semaphore_wait(barrier, peers - 1)

    if tight:
        y, c = lax.div(d, 2), lax.rem(d, 2)
        up = lax.rem(y + 1, 4) * 2 + c
        dn = lax.rem(y + 3, 4) * 2 + c
        opp = lax.rem(y + 2, 4) * 2 + c
        mate = y * 2 + 1 - c
        cols = win_hbm.shape[1]
        half = win_hbm.shape[0] // 2
        pairs = ((win_hbm, win_all), (wout_hbm, wout_all))

        def part(ref, owner, lead=slice(None)):
            return ref.at[lead, pl.ds(pl.multiple_of(owner * cols, cols), cols), :]

        def wcopy(src, dst, sem, target):
            return pltpu.make_async_remote_copy(
                src_ref=src,
                dst_ref=dst,
                send_sem=wsend.at[sem],
                recv_sem=wrecv.at[sem],
                device_id={"mp": m, "dp": target},
                device_id_type=MESH,
            )

        first = [
            wcopy(src, part(dst, d), a * 8 + s, target)
            for a, (src, dst) in enumerate(pairs)
            for s, target in enumerate((up, dn, mate))
        ]
        for copy in first:
            copy.start()
        own_w = [
            pltpu.make_async_copy(src, part(dst, d), wown.at[a]) for a, (src, dst) in enumerate(pairs)
        ]
        for copy in own_w:
            copy.start()

        def need_copy(step):
            return pltpu.make_async_remote_copy(
                src_ref=need_ref,
                dst_ref=mp_need.at[step],
                send_sem=nsend.at[step],
                recv_sem=nrecv.at[step],
                device_id={"mp": lax.rem(m + step, peers), "dp": d},
                device_id_type=MESH,
            )

        def tell(step, carry):
            need_copy(step).start()
            return carry

        lax.fori_loop(1, peers, tell, 0)
    table_copy.wait()

    lane = iota((entries, entries), 1)
    sub = iota((samples, entries), 0)
    wide = iota((entries, RCHUNK), 1)
    deep = iota((space, entries), 0)
    first_row = iota((8, samples), 0) == 0.0
    long = iota((samples, space), 1)

    def send(step):
        return pltpu.make_async_remote_copy(
            src_ref=sbuf.at[step],
            dst_ref=rbuf.at[step],
            send_sem=send_sem.at[step],
            recv_sem=recv_sem.at[step],
            device_id={"mp": ahead(step), "dp": d},
            device_id_type=MESH,
        )

    def fill(step):
        p = ahead(step)
        spread, gathered = [], []
        for j in range(CAP):
            slot = p * CAP + j
            column = jnp.sum(jnp.where(lane == slot.astype(F32), rows_ref[...], 0.0), axis=1, keepdims=True)
            table = tab_ref[0, slot]
            picked = jnp.zeros((entries, width), F32)
            for piece in range(rows_dev // RCHUNK):
                picked += dot(
                    hot(column - float(piece * RCHUNK) == wide),
                    tables_v[table, piece * RCHUNK : (piece + 1) * RCHUNK, :],
                )
            gathered.append(picked.astype(BF16))
            halves = jnp.where(first_row, qh_ref[pl.ds(slot, 1), :], ql_ref[pl.ds(slot, 1), :]).astype(BF16)
            found = dot(halves, hot(slots_ref[pl.ds(slot, 1), :] == sub))
            spread.append(hot(64.0 * found[0:1] + found[1:2] - 1.0 == deep))
        packed = dot(jnp.concatenate(spread, axis=1), jnp.concatenate(gathered, axis=0))
        sbuf[step, :space, :] = packed.astype(BF16)
        sbuf[step, space:, :] = meta_ref[p]

    def body(step, carry):
        fill(step)
        last = step - 1

        @pl.when((step >= 1) & (last != self_step))
        def _():
            send(last).start()

        return carry

    lax.fori_loop(0, peers, body, 0)

    if tight:
        def hear(step, carry):
            need_copy(step).wait_recv()
            return jnp.maximum(carry, mp_need[step])

        mine[...] = lax.fori_loop(1, peers, hear, need_ref[...])

    send(peers - 1).start()

    if tight:

        def flag_copy(step):
            return pltpu.make_async_remote_copy(
                src_ref=mine,
                dst_ref=dp_need.at[step],
                send_sem=dsend.at[step],
                recv_sem=drecv.at[step],
                device_id={"mp": m, "dp": lax.rem(d + step, 8)},
                device_id_type=MESH,
            )

        for step in range(1, 8):
            flag_copy(step).start()

        low, high = slice(0, half), slice(half, 2 * half)
        second = []
        for a, (src, dst) in enumerate(pairs):
            wcopy(src, part(dst, dn), a * 8 + 0, up).wait_recv()
            wcopy(src, part(dst, up), a * 8 + 1, dn).wait_recv()
            second.append(wcopy(part(dst, dn, low), part(dst, dn, low), a * 8 + 3, up))
            second.append(wcopy(part(dst, up, high), part(dst, up, high), a * 8 + 4, dn))
            second.append(wcopy(part(dst, dn), part(dst, dn), a * 8 + 5, mate))
            second.append(wcopy(part(dst, up), part(dst, up), a * 8 + 6, mate))
        for copy in second:
            copy.start()

    def unpack(buf, source, index):
        facts = buf[index, space:, :].astype(F32)[: 2 * CAP]
        facts_ref[source] = facts
        turned = facts.T
        spots = []
        for j in range(CAP):
            code = turned[:, j : j + 1]
            offset = 16.0 * turned[1:2, CAP + j : CAP + j + 1] + turned[2:3, CAP + j : CAP + j + 1]
            spots.append(hot(jnp.where(code > 0.0, code - 1.0 + offset, -1.0) == long))
        got = dot(jnp.concatenate(spots, axis=0), buf[index, :space, :])
        got_ref[source] = got.astype(BF16)

    unpack(sbuf, m, self_step)

    def take(step, carry):
        @pl.when(step != self_step)
        def _():
            pltpu.make_async_remote_copy(
                src_ref=sbuf.at[step],
                dst_ref=rbuf.at[step],
                send_sem=send_sem.at[step],
                recv_sem=recv_sem.at[step],
                device_id={"mp": behind(step), "dp": d},
                device_id_type=MESH,
            ).wait_recv()
            unpack(rbuf, behind(step), step)

        return carry

    if tight:
        lax.fori_loop(0, peers // 2, take, 0)
        third = []
        for a, (src, dst) in enumerate(pairs):
            wcopy(part(dst, opp, low), part(dst, opp, low), a * 8 + 3, up).wait_recv()
            wcopy(part(dst, opp, high), part(dst, opp, high), a * 8 + 4, dn).wait_recv()
            third.append(wcopy(part(dst, opp), part(dst, opp), a * 8 + 7, mate))
        for copy in third:
            copy.start()
        lax.fori_loop(peers // 2, peers, take, 0)
        worst = mine[...]
        for step in range(1, 8):
            flag_copy(step).wait()
            worst = jnp.maximum(worst, dp_need[step])
        flag_ref[...] = worst
        for a, (src, dst) in enumerate(pairs):
            for s in (2, 5, 6, 7):
                wcopy(src, part(dst, mate), a * 8 + s, mate).wait_recv()
        for copy in first + second + third:
            copy.wait_send()
        for copy in own_w:
            copy.wait()

        def told(step, carry):
            need_copy(step).wait_send()
            return carry

        lax.fori_loop(1, peers, told, 0)
    else:
        lax.fori_loop(0, peers, take, 0)

    def sent(step, carry):
        @pl.when(step != self_step)
        def _():
            send(step).wait_send()

        return carry

    lax.fori_loop(0, peers, sent, 0)


def exchange(tight, peers, tables, prepared, weights):
    tab, rows_t, slots_s, q_high, q_low, meta, need = prepared
    table_count, rows_dev, width = tables.shape
    entries, slots_n = rows_t.shape
    space = TIGHT if tight else CAP * entries
    hbm = pl.BlockSpec(memory_space=pl.ANY)
    vmem = pl.BlockSpec(memory_space=pltpu.VMEM)
    sems = pltpu.SemaphoreType.DMA
    operands = [tab, tables, rows_t, slots_s, q_high, q_low, meta.reshape(peers, META, width)]
    in_specs = [pl.BlockSpec(memory_space=pltpu.SMEM), hbm, vmem, vmem, vmem, vmem, vmem]
    out_shape = [
        jax.ShapeDtypeStruct((peers, CAP * entries, width), BF16),
        jax.ShapeDtypeStruct((peers, 2 * CAP, width), F32),
    ]
    out_specs = [vmem, vmem]
    scratch = [
        pltpu.VMEM((table_count, rows_dev, width), BF16),
        pltpu.VMEM((peers, space + META, width), BF16),
        pltpu.VMEM((peers, space + META, width), BF16),
        sems,
        sems((peers,)),
        sems((peers,)),
    ]
    if tight:
        operands += [need, *weights]
        in_specs += [vmem, hbm, hbm]
        out_shape.append(jax.ShapeDtypeStruct(need.shape, F32))
        out_specs.append(vmem)
        for w in weights:
            experts, cols, rank = w.shape
            out_shape.append(jax.ShapeDtypeStruct((experts, cols * lax.axis_size("dp"), rank), BF16))
            out_specs.append(hbm)
        scratch += [
            pltpu.VMEM((peers,) + need.shape, F32),
            pltpu.VMEM((8,) + need.shape, F32),
            pltpu.VMEM(need.shape, F32),
            sems((peers,)),
            sems((peers,)),
            sems((8,)),
            sems((8,)),
            sems((16,)),
            sems((16,)),
            sems((2,)),
        ]
    return pl.pallas_call(
        functools.partial(exchange_kernel, tight, peers),
        out_shape=out_shape,
        in_specs=in_specs,
        out_specs=out_specs,
        scratch_shapes=scratch,
        compiler_params=pltpu.CompilerParams(
            has_side_effects=True, collective_id=0 if tight else 1, vmem_limit_bytes=LIMIT
        ),
        name="exchange_tight" if tight else "exchange_full",
    )(*operands)


def cross_kernel(
    tab_ref, got_ref, mix_ref, bias_ref, gate_ref, win_hbm, wout_hbm, out_ref, acc, win_v, wout_v, sems
):
    peers = got_ref.shape[0]
    samples, wide = acc.shape
    width = got_ref.shape[2]
    experts = win_v.shape[0]
    in_copy = pltpu.make_async_copy(win_hbm, win_v, sems.at[0])
    out_copy = pltpu.make_async_copy(wout_hbm, wout_v, sems.at[1])
    in_copy.start()
    out_copy.start()
    acc[...] = jnp.zeros_like(acc)

    def add(q, carry):
        for j in range(CAP):
            table = tab_ref[q, j] - 1

            @pl.when(table >= 0)
            def _():
                col = pl.ds(pl.multiple_of(table * width, width), width)
                acc[:, col] += got_ref[q, j * samples : (j + 1) * samples, :].astype(F32)

        return carry

    lax.fori_loop(0, peers, add, 0)
    embedded = acc[...].astype(BF16)
    gate = jax.nn.sigmoid(dot_t(embedded, gate_ref[...]))
    in_copy.wait()
    mixed = []
    for e in range(experts):
        hidden = jnp.tanh(dot(embedded, win_v[e])).astype(BF16)
        mixed.append(jnp.tanh(dot(hidden, mix_ref[e])).astype(BF16))
    out_copy.wait()
    span_cols = 512
    for k in range(wide // span_cols):
        span = slice(k * span_cols, (k + 1) * span_cols)
        weighted = jnp.zeros((samples, span_cols), F32)
        for e in range(experts):
            grown = dot_t(mixed[e], wout_v[e, span, :])
            weighted += gate[:, e : e + 1] * (grown + bias_ref[e : e + 1, span])
        base = embedded[:, span].astype(F32)
        out_ref[:, span] = (base + base * weighted).astype(BF16)


def cross(tabs, got, win_all, wout_all, cross_mix, cross_bias, gate_weight):
    samples = got.shape[1] // CAP
    wide = cross_bias.shape[1]
    hbm = pl.BlockSpec(memory_space=pl.ANY)
    vmem = pl.BlockSpec(memory_space=pltpu.VMEM)
    return pl.pallas_call(
        cross_kernel,
        out_shape=jax.ShapeDtypeStruct((samples, wide), BF16),
        in_specs=[pl.BlockSpec(memory_space=pltpu.SMEM), vmem, vmem, vmem, vmem, hbm, hbm],
        out_specs=vmem,
        scratch_shapes=[
            pltpu.VMEM((samples, wide), F32),
            pltpu.VMEM(win_all.shape, BF16),
            pltpu.VMEM(wout_all.shape, BF16),
            pltpu.SemaphoreType.DMA((2,)),
        ],
        compiler_params=pltpu.CompilerParams(vmem_limit_bytes=LIMIT),
        name="cross",
    )(tabs, got, cross_mix, cross_bias, gate_weight, win_all, wout_all)


def on_device(
    tables,
    block_rows,
    block_slots,
    block_table,
    block_peer,
    block_len,
    block_count,
    cross_in,
    cross_mix,
    cross_out,
    cross_bias,
    gate_weight,
):
    peers = lax.axis_size("mp")
    blocks = block_rows.shape[0]
    inputs = (
        block_count,
        block_rows,
        block_slots,
        block_table.reshape(1, blocks),
        block_peer.reshape(1, blocks),
        block_len.reshape(1, blocks),
    )
    prepared = prep(True, peers, *inputs)
    got, facts, flag, win_all, wout_all = exchange(
        True, peers, tables, prepared, (cross_in, cross_out.transpose(0, 2, 1))
    )

    def full():
        return tuple(exchange(False, peers, tables, prep(False, peers, *inputs), ()))

    got, facts = lax.cond(flag[0, 0] > TIGHT, full, lambda: (got, facts))
    tabs = facts[:, CAP:, 0].astype(jnp.int32)
    return cross(tabs, got, win_all, wout_all, cross_mix, cross_bias, gate_weight)


def solution(mesh):
    in_specs = (
        P(None, "mp", None),
        P(("mp", "dp"), None),
        P(("mp", "dp"), None),
        P(("mp", "dp")),
        P(("mp", "dp"), None),
        P(("mp", "dp")),
        P(("mp", "dp")),
        P(None, "dp", None),
        P(),
        P(None, None, "dp"),
        P(),
        P(),
    )
    out_specs = P(("mp", "dp"), None)
    return jax.shard_map(
        on_device, mesh=mesh, in_specs=in_specs, out_specs=out_specs, check_vma=False
    )
```

```python
import functools

import jax
import jax.numpy as jnp
from jax import lax
from jax.experimental import pallas as pl
from jax.experimental.pallas import tpu as pltpu
from jax.sharding import PartitionSpec as P

MESH = pl.DeviceIdType.MESH
F32, BF16 = jnp.float32, jnp.bfloat16
CAP = 4
META = 8
LANE = 240
SPILL = 96
RCHUNK = 512
LIMIT = 60 * 1024 * 1024


def iota(shape, axis):
    return lax.broadcasted_iota(jnp.int32, shape, axis).astype(F32)


def dot(a, b):
    return jnp.dot(a, b, preferred_element_type=F32)


def dot_t(a, b):
    return lax.dot_general(a, b, (((1,), (1,)), ((), ())), preferred_element_type=F32)


def dot_l(a, b):
    return lax.dot_general(a, b, (((0,), (0,)), ((), ())), preferred_element_type=F32)


def hot(mask):
    return jnp.where(mask, 1.0, 0.0).astype(BF16)


def prep_kernel(
    tight, count_ref, rows_ref, slots_ref, table_ref, peer_ref, len_ref, tab_o, rows_o, slots_o, qh_o, ql_o, meta_o, need_o, used
):
    blocks, entries = rows_ref.shape
    slots_n = rows_o.shape[1]
    count = count_ref[0].astype(F32)
    k_sub, k_lane = iota((blocks, blocks), 0), iota((blocks, blocks), 1)
    eye = k_sub == k_lane

    def column(row):
        return jnp.sum(jnp.where(eye, row, 0.0), axis=1, keepdims=True)

    table_r, peer_r = table_ref[...].astype(F32), peer_ref[...].astype(F32)
    table_c, peer_c, len_c = column(table_r), column(peer_r), column(len_ref[...].astype(F32))
    live_r, live_c = k_lane[:1] < count, k_sub[:, :1] < count
    same = peer_c == peer_r
    before = same & (k_lane < k_sub)
    alike = same & (column(table_r) == table_r) & live_r & live_c
    follows_c = jnp.max(jnp.where(alike & (k_lane < k_sub), 1.0, 0.0), axis=1, keepdims=True)
    follows_r = jnp.max(jnp.where(alike & (k_sub < k_lane), 1.0, 0.0), axis=0, keepdims=True)
    leads_c = jnp.where(live_c, 1.0 - follows_c, 0.0)
    pos_c = jnp.sum(jnp.where(before, 1.0, 0.0), axis=1, keepdims=True)
    pos_r = jnp.sum(jnp.where(same & (k_sub < k_lane), 1.0, 0.0), axis=0, keepdims=True)
    target_r = jnp.where(live_r, peer_r * CAP + pos_r, -1.0)
    target_c = jnp.where(live_c, peer_c * CAP + pos_c, -1.0)
    place = hot(iota((slots_n, blocks), 0) == target_r)
    place_t = hot(target_c == iota((blocks, slots_n), 1))

    live_entry = (iota((blocks, entries), 1) < len_c) & live_c
    slot_code = jnp.where(live_entry, slots_ref[...].astype(F32) + 1.0, 0.0)
    slots_o[...] = dot(place, slot_code.astype(BF16)) - 1.0
    row_code = jnp.where(live_entry, rows_ref[...].astype(F32) + 1.0, 0.0)
    high = jnp.floor(row_code * (1.0 / 64.0))
    low = row_code - 64.0 * high
    rows_o[...] = 64.0 * dot_l(high.astype(BF16), place_t) + dot_l(low.astype(BF16), place_t) - 1.0
    tab_o[...] = dot(jnp.broadcast_to(table_r, (8, blocks)).astype(BF16), place_t).astype(jnp.int32)

    lanes = iota((entries, entries), 1)
    if tight:
        slot_t = slot_code.T - 1.0
        for k in range(blocks):
            touched = jnp.where(slot_t[:, k : k + 1] == lanes, 1.0, 0.0)
            used[k : k + 1, :] = jnp.minimum(jnp.sum(touched, axis=0, keepdims=True), 1.0)
        taken = leads_c * jnp.minimum(dot(hot(alike), used[...].astype(BF16)), 1.0)
    else:
        taken = leads_c + jnp.zeros((blocks, entries), F32)
    rank = dot(taken.astype(BF16), hot(iota((entries, entries), 0) < lanes))
    amount_c = jnp.sum(taken, axis=1, keepdims=True)
    amount_r = jnp.sum(jnp.where(eye, amount_c, 0.0), axis=0, keepdims=True)
    off_c = jnp.sum(jnp.where(before, amount_r, 0.0), axis=1, keepdims=True)
    need_o[...] = jnp.zeros_like(need_o) + jnp.sum(
        jnp.where(peer_c == iota((blocks, entries), 1), amount_c, 0.0), axis=0, keepdims=True
    )

    spot = jnp.where(taken > 0.0, off_c + rank + 1.0, 0.0)
    spot_high = jnp.floor(spot * (1.0 / 64.0))
    spot_low = spot - 64.0 * spot_high
    led = hot(alike & (follows_r == 0.0))
    qh_o[...] = dot(place, dot(led, spot_high.astype(BF16)).astype(BF16))
    ql_o[...] = dot(place, dot(led, spot_low.astype(BF16)).astype(BF16))

    off_high = jnp.floor(off_c * (1.0 / 16.0))
    lane_e = iota((blocks, entries), 1)
    facts = jnp.where(lane_e == 0.0, table_c + 1.0, jnp.where(lane_e == 1.0, off_high, off_c - 16.0 * off_high))
    facts = jnp.where(lane_e < 3.0, leads_c * facts, 0.0)
    line = lax.broadcasted_iota(jnp.int32, (meta_o.shape[0], blocks), 0)
    pair, part = (line >> 3) * CAP, line & 7
    rank_line = hot(jnp.where(part < CAP, pair + part, -2).astype(F32) == target_r)
    fact_line = hot(jnp.where((part >= CAP) & (part < 2 * CAP), pair + part - CAP, -2).astype(F32) == target_r)
    meta = dot(rank_line, (taken * (rank + 1.0)).astype(BF16)) + dot(fact_line, facts.astype(BF16))
    meta_o[...] = meta.astype(BF16)


def prep(tight, peers, count, rows, slots, table, peer, length):
    blocks, entries = rows.shape
    slots_n = peers * CAP
    vmem = pl.BlockSpec(memory_space=pltpu.VMEM)
    return pl.pallas_call(
        functools.partial(prep_kernel, tight),
        out_shape=(
            jax.ShapeDtypeStruct((8, slots_n), jnp.int32),
            jax.ShapeDtypeStruct((entries, slots_n), F32),
            jax.ShapeDtypeStruct((slots_n, entries), F32),
            jax.ShapeDtypeStruct((slots_n, entries), F32),
            jax.ShapeDtypeStruct((slots_n, entries), F32),
            jax.ShapeDtypeStruct((peers * META, entries), BF16),
            jax.ShapeDtypeStruct((8, entries), F32),
        ),
        in_specs=[pl.BlockSpec(memory_space=pltpu.SMEM)] + [vmem] * 5,
        out_specs=(vmem,) * 7,
        scratch_shapes=[pltpu.VMEM((blocks, entries), F32)],
        name="prep_tight" if tight else "prep_full",
    )(count, rows, slots, table, peer, length)


def exchange_kernel(tight, peers, *refs):
    if tight:
        (tab_hbm, tables_hbm, rows_ref, slots_ref, qh_ref, ql_ref, meta_ref, need_ref, win_hbm, wout_hbm) = refs[:10]
        (got_ref, facts_ref, flag_ref, win_all, wout_all) = refs[10:15]
        (tables_v, sbuf, rbuf, tab_ref, table_sem, tab_sem, send_sem, recv_sem) = refs[15:23]
        (mp_need, dp_need, mate_need, wish, mine, nsend, nrecv, dsend, drecv) = refs[23:32]
        (wsend, wrecv, wown, over, under, back, osend, orecv, bsend, brecv) = refs[32:]
    else:
        (tab_hbm, tables_hbm, rows_ref, slots_ref, qh_ref, ql_ref, meta_ref) = refs[:7]
        (got_ref, facts_ref) = refs[7:9]
        (tables_v, sbuf, rbuf, tab_ref, table_sem, tab_sem, send_sem, recv_sem) = refs[9:]
    m = lax.axis_index("mp")
    d = lax.axis_index("dp")
    table_count, rows_dev, width = tables_v.shape
    entries = rows_ref.shape[0]
    samples = entries
    space = sbuf.shape[1] - META
    spill = SPILL if tight else 0
    room = space + spill
    x, z = lax.div(m, 8), lax.rem(m, 8)
    self_step = peers - 1

    def shift(step):
        turn = lax.rem(step + 1, peers)
        return lax.div(turn, 8), lax.rem(turn, 8)

    def ahead(step):
        dx, dz = shift(step)
        return lax.rem(x + dx, 4) * 8 + lax.rem(z + dz, 8)

    def behind(step):
        dx, dz = shift(step)
        return lax.rem(x + 4 - dx, 4) * 8 + lax.rem(z + 8 - dz, 8)

    table_copy = pltpu.make_async_copy(tables_hbm, tables_v, table_sem)
    table_copy.start()
    tab_copy = pltpu.make_async_copy(tab_hbm, tab_ref, tab_sem)
    tab_copy.start()

    barrier = pltpu.get_barrier_semaphore()

    def greet(step, carry):
        pl.semaphore_signal(
            barrier, inc=1, device_id={"mp": lax.rem(m + step, peers), "dp": d}, device_id_type=MESH
        )
        return carry

    lax.fori_loop(1, peers, greet, 0)
    if tight:
        for step in range(1, 8):
            pl.semaphore_signal(
                barrier, inc=1, device_id={"mp": m, "dp": lax.rem(d + step, 8)}, device_id_type=MESH
            )
        pl.semaphore_wait(barrier, peers - 1 + 7)
    else:
        pl.semaphore_wait(barrier, peers - 1)

    if tight:
        y, c = lax.div(d, 2), lax.rem(d, 2)
        up = lax.rem(y + 1, 4) * 2 + c
        dn = lax.rem(y + 3, 4) * 2 + c
        opp = lax.rem(y + 2, 4) * 2 + c
        mate = y * 2 + 1 - c
        cols = win_hbm.shape[1]
        half = win_hbm.shape[0] // 2
        pairs = ((win_hbm, win_all), (wout_hbm, wout_all))

        def part(ref, owner, lead=slice(None)):
            return ref.at[lead, pl.ds(pl.multiple_of(owner * cols, cols), cols), :]

        def wcopy(src, dst, sem, target):
            return pltpu.make_async_remote_copy(
                src_ref=src,
                dst_ref=dst,
                send_sem=wsend.at[sem],
                recv_sem=wrecv.at[sem],
                device_id={"mp": m, "dp": target},
                device_id_type=MESH,
            )

        low, high = slice(0, half), slice(half, 2 * half)
        first = []
        for kinds in (((0, low, up), (2, high, dn)), ((1, high, up), (3, low, dn)), ((4, slice(0, 2 * half), mate),)):
            for a, (src, dst) in enumerate(pairs):
                for kind, lead, target in kinds:
                    first.append(wcopy(src.at[lead], part(dst, d, lead), a * 10 + kind, target))
        for copy in first:
            copy.start()

        def heard(kinds):
            for a, (src, dst) in enumerate(pairs):
                for kind, owner, lead in kinds:
                    wcopy(part(dst, owner, lead), part(dst, owner, lead), a * 10 + kind, mate).wait_recv()

        def passed(kinds):
            return [
                wcopy(part(dst, owner, lead), part(dst, owner, lead), a * 10 + kind, target)
                for a, (src, dst) in enumerate(pairs)
                for kind, owner, lead, target in kinds
            ]

        whole = slice(0, 2 * half)
        second = ((5, dn, low, up), (6, up, high, dn))
        third = ((7, dn, whole, mate), (8, up, whole, mate))
        fourth = ((9, opp, whole, mate),)
        own_w = [
            pltpu.make_async_copy(src, part(dst, d), wown.at[a]) for a, (src, dst) in enumerate(pairs)
        ]
        for copy in own_w:
            copy.start()

        mate_copy = pltpu.make_async_remote_copy(
            src_ref=need_ref,
            dst_ref=mate_need,
            send_sem=dsend.at[0],
            recv_sem=drecv.at[0],
            device_id={"mp": m, "dp": mate},
            device_id_type=MESH,
        )
        mate_copy.start()

        def need_copy(step):
            return pltpu.make_async_remote_copy(
                src_ref=wish,
                dst_ref=mp_need.at[step],
                send_sem=nsend.at[step],
                recv_sem=nrecv.at[step],
                device_id={"mp": lax.rem(m + step, peers), "dp": d},
                device_id_type=MESH,
            )

        def tell(step, carry):
            need_copy(step).start()
            return carry

    tab_copy.wait()
    table_copy.wait()

    lane = iota((entries, entries), 1)
    sub = iota((samples, entries), 0)
    wide = iota((entries, RCHUNK), 1)
    def order(where):
        return jnp.where(where < float(space), where, float(2 * space + spill - 1) - where)

    deep = order(iota((room, entries), 0))
    first_row = iota((8, samples), 0) == 0.0
    long = order(iota((samples, room), 1))

    def send(step):
        return pltpu.make_async_remote_copy(
            src_ref=sbuf.at[step],
            dst_ref=rbuf.at[step],
            send_sem=send_sem.at[step],
            recv_sem=recv_sem.at[step],
            device_id={"mp": ahead(step), "dp": d},
            device_id_type=MESH,
        )

    def fill(step):
        p = ahead(step)
        spread, gathered = [], []
        for j in range(CAP):
            slot = p * CAP + j
            column = jnp.sum(jnp.where(lane == slot.astype(F32), rows_ref[...], 0.0), axis=1, keepdims=True)
            table = tab_ref[0, slot]
            picked = jnp.zeros((entries, width), F32)
            for piece in range(rows_dev // RCHUNK):
                picked += dot(
                    hot(column - float(piece * RCHUNK) == wide),
                    tables_v[table, piece * RCHUNK : (piece + 1) * RCHUNK, :],
                )
            gathered.append(picked.astype(BF16))
            halves = jnp.where(first_row, qh_ref[pl.ds(slot, 1), :], ql_ref[pl.ds(slot, 1), :]).astype(BF16)
            found = dot(halves, hot(slots_ref[pl.ds(slot, 1), :] == sub))
            spread.append(hot(64.0 * found[0:1] + found[1:2] - 1.0 == deep))
        packed = dot(jnp.concatenate(spread, axis=1), jnp.concatenate(gathered, axis=0))
        packed = packed.astype(BF16)
        sbuf[step, :space, :] = packed[:space]
        sbuf[step, space:, :] = meta_ref[p]
        if tight:
            over[step] = packed[space:]

    if tight:

        def over_copy(step):
            return pltpu.make_async_remote_copy(
                src_ref=over.at[step],
                dst_ref=under.at[step],
                send_sem=osend.at[step],
                recv_sem=orecv.at[step],
                device_id={"mp": m, "dp": mate},
                device_id_type=MESH,
            )

        def merge(step):
            over_copy(step).wait_recv()
            sbuf[step, space - spill : space, :] = sbuf[step, space - spill : space, :] + under[step]

    lag = 3 if tight else 1

    def body(step, carry):
        @pl.when(step < peers)
        def _():
            fill(step)

        if tight:

            @pl.when(step == 1)
            def _():
                mate_copy.wait()
                wish[...] = jnp.maximum(0.5 * (need_ref[...] + mate_need[...]), need_ref[...] - float(spill))

            @pl.when(step == 3)
            def _():
                lax.fori_loop(1, peers, tell, 0)

            @pl.when(step == peers * 5 // 8)
            def _():
                heard(((0, dn, low), (2, up, high)))
                for copy in passed(second):
                    copy.start()

            @pl.when((step >= 1) & (step <= peers))
            def _():
                over_copy(step - 1).start()

            @pl.when((step >= 2) & (step <= peers + 1))
            def _():
                merge(step - 2)

        last = step - lag

        @pl.when((last >= 0) & (last != self_step))
        def _():
            send(last).start()

        return carry

    lax.fori_loop(0, peers + lag, body, 0)

    if tight:
        def hear(step, carry):
            need_copy(step).wait_recv()
            return jnp.maximum(carry, mp_need[step])

        mine[...] = lax.fori_loop(1, peers, hear, wish[...])

    if tight:

        def flag_copy(step):
            return pltpu.make_async_remote_copy(
                src_ref=mine,
                dst_ref=dp_need.at[step],
                send_sem=dsend.at[step],
                recv_sem=drecv.at[step],
                device_id={"mp": m, "dp": lax.rem(d + step, 8)},
                device_id_type=MESH,
            )

        for step in range(1, 8):
            flag_copy(step).start()

        heard(((1, dn, high), (3, up, low)))
        for copy in passed(third):
            copy.start()

    def unpack(buf, source, index):
        turned = buf[index, space:, :].astype(F32)[: 2 * CAP].T
        facts_ref[pl.ds(source, 1), :] = turned[0:1, :]
        spots = []
        for j in range(CAP):
            code = turned[:, j : j + 1]
            offset = 16.0 * turned[1:2, CAP + j : CAP + j + 1] + turned[2:3, CAP + j : CAP + j + 1]
            spots.append(hot(jnp.where(code > 0.0, code - 1.0 + offset, -1.0) == long))
        held = buf[index, :space, :]
        if tight:
            back_copy(step=index, buf=buf).wait_recv()
            held = jnp.concatenate([held, back[index]], axis=0)
        got = dot(jnp.concatenate(spots, axis=0), held)
        got_ref[source] = got.astype(BF16)

    if tight:

        def back_copy(step, buf):
            return pltpu.make_async_remote_copy(
                src_ref=buf.at[step, space - spill : space, :],
                dst_ref=back.at[step],
                send_sem=bsend.at[step],
                recv_sem=brecv.at[step],
                device_id={"mp": m, "dp": mate},
                device_id_type=MESH,
            )

        back_copy(self_step, sbuf).start()

    behind_by = 3 if tight else 0

    def take(step, carry):
        @pl.when((step != self_step) & (step < peers))
        def _():
            pltpu.make_async_remote_copy(
                src_ref=sbuf.at[step],
                dst_ref=rbuf.at[step],
                send_sem=send_sem.at[step],
                recv_sem=recv_sem.at[step],
                device_id={"mp": behind(step), "dp": d},
                device_id_type=MESH,
            ).wait_recv()
            if tight:
                back_copy(step, rbuf).start()

        ready = step - behind_by

        @pl.when((ready >= 0) & (ready != self_step))
        def _():
            unpack(rbuf, behind(ready), ready)

        return carry

    if tight:
        unpack(sbuf, m, self_step)
        lax.fori_loop(0, peers * 3 // 4, take, 0)
        heard(((5, opp, low), (6, opp, high)))
        for copy in passed(fourth):
            copy.start()
        lax.fori_loop(peers * 3 // 4, peers + behind_by, take, 0)
        worst = mine[...]
        for step in range(1, 8):
            flag_copy(step).wait()
            worst = jnp.maximum(worst, dp_need[step])
        flag_ref[...] = jnp.zeros_like(worst) + jnp.max(worst, axis=1, keepdims=True)
        heard(((4, mate, whole), (7, mate, whole), (8, mate, whole), (9, mate, whole)))
        for copy in first + passed(second) + passed(third) + passed(fourth):
            copy.wait_send()
        for copy in own_w:
            copy.wait()

        def told(step, carry):
            need_copy(step).wait_send()
            return carry

        lax.fori_loop(1, peers, told, 0)

        def drained(step, carry):
            over_copy(step).wait_send()
            back_copy(step, rbuf).wait_send()
            return carry

        lax.fori_loop(0, peers, drained, 0)
    else:
        unpack(sbuf, m, self_step)
        lax.fori_loop(0, peers, take, 0)

    def sent(step, carry):
        @pl.when(step != self_step)
        def _():
            send(step).wait_send()

        return carry

    lax.fori_loop(0, peers, sent, 0)


def exchange(tight, peers, tables, prepared, weights):
    tab, rows_t, slots_s, q_high, q_low, meta, need = prepared
    table_count, rows_dev, width = tables.shape
    entries, slots_n = rows_t.shape
    space = LANE if tight else CAP * entries
    hbm = pl.BlockSpec(memory_space=pl.ANY)
    vmem = pl.BlockSpec(memory_space=pltpu.VMEM)
    sems = pltpu.SemaphoreType.DMA
    operands = [tab, tables, rows_t, slots_s, q_high, q_low, meta.reshape(peers, META, width)]
    in_specs = [hbm, hbm, vmem, vmem, vmem, vmem, vmem]
    out_shape = [
        jax.ShapeDtypeStruct((peers, CAP * entries, width), BF16),
        jax.ShapeDtypeStruct((peers, 2 * CAP), F32),
    ]
    out_specs = [vmem, vmem]
    scratch = [
        pltpu.VMEM((table_count, rows_dev, width), BF16),
        pltpu.VMEM((peers, space + META, width), BF16),
        pltpu.VMEM((peers, space + META, width), BF16),
        pltpu.SMEM(tab.shape, jnp.int32),
        sems,
        sems,
        sems((peers,)),
        sems((peers,)),
    ]
    if tight:
        operands += [need, *weights]
        in_specs += [vmem, hbm, hbm]
        out_shape.append(jax.ShapeDtypeStruct(need.shape, F32))
        out_specs.append(vmem)
        for w in weights:
            experts, cols, rank = w.shape
            out_shape.append(jax.ShapeDtypeStruct((experts, cols * lax.axis_size("dp"), rank), BF16))
            out_specs.append(hbm)
        scratch += [
            pltpu.VMEM((peers,) + need.shape, F32),
            pltpu.VMEM((8,) + need.shape, F32),
            pltpu.VMEM(need.shape, F32),
            pltpu.VMEM(need.shape, F32),
            pltpu.VMEM(need.shape, F32),
            sems((peers,)),
            sems((peers,)),
            sems((8,)),
            sems((8,)),
            sems((20,)),
            sems((20,)),
            sems((2,)),
            pltpu.VMEM((peers, SPILL, width), BF16),
            pltpu.VMEM((peers, SPILL, width), BF16),
            pltpu.VMEM((peers, SPILL, width), BF16),
            sems((peers,)),
            sems((peers,)),
            sems((peers,)),
            sems((peers,)),
        ]
    return pl.pallas_call(
        functools.partial(exchange_kernel, tight, peers),
        out_shape=out_shape,
        in_specs=in_specs,
        out_specs=out_specs,
        scratch_shapes=scratch,
        compiler_params=pltpu.CompilerParams(
            has_side_effects=True, collective_id=0 if tight else 1, vmem_limit_bytes=LIMIT
        ),
        name="exchange_tight" if tight else "exchange_full",
    )(*operands)


def cross_kernel(
    facts_hbm, got_ref, mix_ref, bias_ref, gate_ref, win_hbm, wout_hbm, out_ref, acc, win_v, wout_v, facts, sems
):
    peers = got_ref.shape[0]
    samples, wide = acc.shape
    width = got_ref.shape[2]
    experts = win_v.shape[0]
    in_copy = pltpu.make_async_copy(win_hbm, win_v, sems.at[0])
    out_copy = pltpu.make_async_copy(wout_hbm, wout_v, sems.at[1])
    facts_copy = pltpu.make_async_copy(facts_hbm, facts, sems.at[2])
    facts_copy.start()
    in_copy.start()
    out_copy.start()
    acc[...] = jnp.zeros_like(acc)
    facts_copy.wait()

    def add(q, carry):
        for j in range(CAP):
            table = facts[q, CAP + j].astype(jnp.int32) - 1

            @pl.when(table >= 0)
            def _():
                col = pl.ds(pl.multiple_of(table * width, width), width)
                acc[:, col] += got_ref[q, j * samples : (j + 1) * samples, :].astype(F32)

        return carry

    lax.fori_loop(0, peers, add, 0)
    embedded = acc[...].astype(BF16)
    gate = jax.nn.sigmoid(dot_t(embedded, gate_ref[...]))
    in_copy.wait()
    mixed = []
    for e in range(experts):
        hidden = jnp.tanh(dot(embedded, win_v[e])).astype(BF16)
        mixed.append(jnp.tanh(dot(hidden, mix_ref[e])).astype(BF16))
    out_copy.wait()
    span_cols = 512
    for k in range(wide // span_cols):
        span = slice(k * span_cols, (k + 1) * span_cols)
        weighted = jnp.zeros((samples, span_cols), F32)
        for e in range(experts):
            grown = dot_t(mixed[e], wout_v[e, span, :])
            weighted += gate[:, e : e + 1] * (grown + bias_ref[e : e + 1, span])
        base = embedded[:, span].astype(F32)
        out_ref[:, span] = (base + base * weighted).astype(BF16)


def cross(facts, got, win_all, wout_all, cross_mix, cross_bias, gate_weight):
    samples = got.shape[1] // CAP
    wide = cross_bias.shape[1]
    hbm = pl.BlockSpec(memory_space=pl.ANY)
    vmem = pl.BlockSpec(memory_space=pltpu.VMEM)
    return pl.pallas_call(
        cross_kernel,
        out_shape=jax.ShapeDtypeStruct((samples, wide), BF16),
        in_specs=[hbm, vmem, vmem, vmem, vmem, hbm, hbm],
        out_specs=vmem,
        scratch_shapes=[
            pltpu.VMEM((samples, wide), F32),
            pltpu.VMEM(win_all.shape, BF16),
            pltpu.VMEM(wout_all.shape, BF16),
            pltpu.SMEM(facts.shape, F32),
            pltpu.SemaphoreType.DMA((3,)),
        ],
        compiler_params=pltpu.CompilerParams(vmem_limit_bytes=LIMIT),
        name="cross",
    )(facts, got, cross_mix, cross_bias, gate_weight, win_all, wout_all)


def on_device(
    tables,
    block_rows,
    block_slots,
    block_table,
    block_peer,
    block_len,
    block_count,
    cross_in,
    cross_mix,
    cross_out,
    cross_bias,
    gate_weight,
):
    peers = lax.axis_size("mp")
    blocks = block_rows.shape[0]
    inputs = (
        block_count,
        block_rows,
        block_slots,
        block_table.reshape(1, blocks),
        block_peer.reshape(1, blocks),
        block_len.reshape(1, blocks),
    )
    prepared = prep(True, peers, *inputs)
    got, facts, flag, win_all, wout_all = exchange(
        True, peers, tables, prepared, (cross_in, cross_out.transpose(0, 2, 1))
    )

    def full():
        return tuple(exchange(False, peers, tables, prep(False, peers, *inputs), ()))

    got, facts = lax.cond(flag[0, 0] > LANE, full, lambda: (got, facts))
    return cross(facts, got, win_all, wout_all, cross_mix, cross_bias, gate_weight)


def solution(mesh):
    in_specs = (
        P(None, "mp", None),
        P(("mp", "dp"), None),
        P(("mp", "dp"), None),
        P(("mp", "dp")),
        P(("mp", "dp"), None),
        P(("mp", "dp")),
        P(("mp", "dp")),
        P(None, "dp", None),
        P(),
        P(None, None, "dp"),
        P(),
        P(),
    )
    out_specs = P(("mp", "dp"), None)
    return jax.shard_map(
        on_device, mesh=mesh, in_specs=in_specs, out_specs=out_specs, check_vma=False
    )
```
